32 devices in a mesh: beam: 2 (over x), pulse: 16 (over z, y, core).
Axes of the slice: x: 2, y: 2, z: 4, core: 2. Of those that a mesh axis runs over, the one named last changes fastest.
Arguments:
- echoes: float32 [2, 4096, 1536], P(None, 'pulse', 'beam'), parts along dimension 2, may hold values from -6 to 6
- guard_gates: int32 [1], replicated, may hold values from 1 to 4
- train_gates: int32 [1], replicated, may hold values from 4 to 16
Outputs:
- powers: float32 [4096, 1536], P('pulse', 'beam'), parts along dimension 1
- statistic: float32 [4096, 1536], P('pulse', 'beam'), parts along dimension 1
The draws below stay inside these ranges and needn't reach their ends.
There are 2 independent parts, one for each index of `beam`. The reference program is written for one: setup_inputs(seed, part) draws one part's arguments, and reference() takes and returns one part's arrays. A program takes and returns all parts, laid end to end along the dimension named above; an argument that names none is the same for every part. Nothing has to cross between parts.
All inputs are finite; a program needn't handle non-finite values.
Results may differ from the reference program's by a relative error of at most 0.0003.
Values sent between devices are 32-bit elements; how exact they have to be, the bound alone decides.
No kernel may reach another device: no remote copies, remote signals or barrier semaphores. Data moves between devices by JAX's collectives and lax.ppermute only.
A program may use at most 192 MiB of HBM per device.

```python
import jax
import jax.numpy as jnp
from jax import lax

PULSES = 4096
GATES = 768
GUARD_BINS = 2
TRAIN_BINS = 4


def block_scale(rng, dims, split, smallest, largest):
    level, own = 1.0, jax.random.fold_in(rng, 6)
    for dim, shards_of in split:
        steps = jnp.exp(jax.random.uniform(jax.random.fold_in(own, dim), (shards_of,), jnp.float32, smallest / len(split), largest / len(split)))
        level = level * jnp.repeat(steps, dims[dim] // shards_of).reshape([-1 if axis == dim else 1 for axis in range(len(dims))])
    return level


def centred(rng, dims, scale, limit, pieces=(), kind=jnp.bfloat16):
    array = jax.random.normal(rng, dims, jnp.float32) * scale
    if len(pieces) > 0:
        array = block_scale(rng, dims, pieces, -0.22, 0.18) * array
    return jnp.clip(array, min=-limit, max=limit).astype(kind)


def setup_inputs(seed: int = 0, part: int = 0) -> dict:
    keys = jax.random.split(jax.random.key(seed), 4)
    part_splits = jax.random.split(jax.random.fold_in(keys[3], part), 4)
    return {
        "echoes": centred(part_splits[0], (2, PULSES, GATES), 1.0, 6.0, ((1, 16),), jnp.float32),
        "guard_gates": jax.random.randint(keys[1], (1,), 1, 5).astype(jnp.int32),
        "train_gates": jax.random.randint(keys[2], (1,), 4, 17).astype(jnp.int32),
    }


TWO_PI = 6.283185307179586

def tables(bin_first, bin_count, pulse_first, pulse_count):
    bin_ids = bin_first + jnp.arange(bin_count, dtype=jnp.int32)
    pulse_ids = pulse_first + jnp.arange(pulse_count, dtype=jnp.int32)
    phases = (bin_ids[:, None] * pulse_ids[None, :] % PULSES).astype(jnp.float32) * (TWO_PI / PULSES)
    return (jnp.cos(phases), jnp.sin(phases))

def transform(cosine, sine, samples):
    width = samples.shape[2]
    stacked = jnp.concatenate([samples[0], samples[1]], axis=1)
    first_part = jnp.dot(cosine, stacked, precision=lax.Precision.HIGHEST, preferred_element_type=jnp.float32)
    second_part = jnp.dot(sine, stacked, precision=lax.Precision.HIGHEST, preferred_element_type=jnp.float32)
    real_part = first_part[:, :width] + second_part[:, width:]
    imag_part = first_part[:, width:] - second_part[:, :width]
    return (real_part, imag_part)

def reference(echoes, guard_gates, train_gates):
    scale_factor = 1.0 / jnp.sqrt(jnp.float32(PULSES))

    def one_block(bin_first):
        cosine, sine = tables(bin_first, 512, 0, PULSES)
        real_part, imag_part = transform(cosine, sine, echoes)
        real_part = real_part * scale_factor
        imag_part = imag_part * scale_factor
        return real_part * real_part + imag_part * imag_part
    starts = jnp.arange(PULSES // 512, dtype=jnp.int32) * 512
    powers = lax.map(one_block, starts).reshape(PULSES, GATES)
    guard_width = guard_gates[0]
    train_width = train_gates[0]
    gate_ids = jnp.arange(GATES, dtype=jnp.int32)
    offsets = jnp.abs(gate_ids[:, None] - gate_ids[None, :])
    band = ((offsets > guard_width) & (offsets <= guard_width + train_width)).astype(jnp.float32)
    range_sum = jnp.dot(powers, band, precision=lax.Precision.HIGHEST, preferred_element_type=jnp.float32)
    range_count = lax.optimization_barrier(jnp.sum(band, axis=0))
    doppler_sum = jnp.zeros_like(powers)
    for shift_bins in range(GUARD_BINS + 1, GUARD_BINS + TRAIN_BINS + 1):
        doppler_sum = doppler_sum + jnp.roll(powers, -shift_bins, axis=0) + jnp.roll(powers, shift_bins, axis=0)
    noise_level = (range_sum + doppler_sum) / (range_count[None, :] + 2.0 * TRAIN_BINS)
    statistic = powers / (noise_level + 1.0)
    return (powers, statistic)
```

```python
import jax
import jax.numpy as jnp
import numpy as np
from jax import lax
from jax.experimental import pallas as pl
from jax.experimental.pallas import tpu as pltpu
from jax.sharding import PartitionSpec as P

PULSES = 4096
GUARD_BINS = 2
TRAIN_BINS = 4
LANES = 128
SUBLANES = 8
EDGE = 8
CHUNKS = (3, 3)


TWO_PI = 6.283185307179586


def padded_2(cells, sides, width):
    for axis, dim in sides:
        count = lax.axis_size(axis)
        head = lax.slice_in_dim(cells, 0, width, axis=dim)
        tail = lax.slice_in_dim(cells, cells.shape[dim] - width, cells.shape[dim], axis=dim)
        cells = jnp.concatenate(
            [
                lax.ppermute(tail, axis, [(i, (i + 1) % count) for i in range(count)]),
                cells,
                lax.ppermute(head, axis, [((i + 1) % count, i) for i in range(count)]),
            ],
            axis=dim,
        )
    return cells


def small_tables(count):
    index_row = jnp.arange(count, dtype=jnp.int32)
    phases = (index_row[:, None] * index_row[None, :] % count).astype(jnp.float32) * (
        TWO_PI / count
    )
    return (jnp.cos(phases), jnp.sin(phases))


def product(left, right):
    return jnp.dot(left, right, precision=lax.Precision.HIGHEST, preferred_element_type=jnp.float32)


def factored_powers(samples):
    width = samples.shape[2]
    bit_count = PULSES.bit_length() - 1
    first_radix = 2 ** (bit_count // 2)
    second_radix = PULSES // first_radix
    cos_first, sin_first = small_tables(first_radix)
    real_in = samples[0].reshape(first_radix, second_radix * width)
    imag_in = samples[1].reshape(first_radix, second_radix * width)
    real_one = (product(cos_first, real_in) + product(sin_first, imag_in)).reshape(
        first_radix, second_radix, width
    )
    imag_one = (product(cos_first, imag_in) - product(sin_first, real_in)).reshape(
        first_radix, second_radix, width
    )
    first_ids = jnp.arange(first_radix, dtype=jnp.int32)
    second_ids = jnp.arange(second_radix, dtype=jnp.int32)
    twist = (first_ids[:, None] * second_ids[None, :] % PULSES).astype(jnp.float32) * (
        TWO_PI / PULSES
    )
    twist_cos = jnp.cos(twist)[:, :, None]
    twist_sin = jnp.sin(twist)[:, :, None]
    real_two = twist_cos * real_one + twist_sin * imag_one
    imag_two = twist_cos * imag_one - twist_sin * real_one
    real_two = jnp.transpose(real_two, (1, 0, 2)).reshape(second_radix, first_radix * width)
    imag_two = jnp.transpose(imag_two, (1, 0, 2)).reshape(second_radix, first_radix * width)
    cos_second, sin_second = small_tables(second_radix)
    scale_factor = 1.0 / jnp.sqrt(jnp.float32(PULSES))
    real_out = (product(cos_second, real_two) + product(sin_second, imag_two)) * scale_factor
    imag_out = (product(cos_second, imag_two) - product(sin_second, real_two)) * scale_factor
    result = real_out * real_out + imag_out * imag_out
    return result.reshape(PULSES, width)


def plain_shards(echoes, guard_gates, train_gates):
    devices_count = lax.axis_size("pulse")
    bins_local = PULSES // devices_count
    gates_count = echoes.shape[2]
    columns = factored_powers(
        lax.all_to_all(echoes, "pulse", split_axis=2, concat_axis=1, tiled=True)
    )
    powers = lax.all_to_all(columns, "pulse", split_axis=0, concat_axis=1, tiled=True)
    reach = GUARD_BINS + TRAIN_BINS
    padded = padded_2(powers, (("pulse", 0),), reach)
    doppler_sum = jnp.zeros_like(powers)
    for shift_bins in range(GUARD_BINS + 1, reach + 1):
        above = padded[reach + shift_bins : reach + shift_bins + bins_local]
        below = padded[reach - shift_bins : reach - shift_bins + bins_local]
        doppler_sum = doppler_sum + above + below
    guard_width = guard_gates[0]
    train_width = train_gates[0]
    gate_ids = jnp.arange(gates_count, dtype=jnp.int32)
    offsets = jnp.abs(gate_ids[:, None] - gate_ids[None, :])
    band = ((offsets > guard_width) & (offsets <= guard_width + train_width)).astype(jnp.float32)
    range_sum = jnp.dot(
        powers, band, precision=lax.Precision.HIGHEST, preferred_element_type=jnp.float32
    )
    range_count = jnp.sum(band, axis=0)
    noise_level = (range_sum + doppler_sum) / (range_count[None, :] + 2.0 * TRAIN_BINS)
    statistic = powers / (noise_level + 1.0)
    return (powers, statistic)


def host_tables(devices, local):
    q = np.arange(local)
    angle = 2.0 * np.pi * np.outer(np.arange(devices), q) / PULSES
    scale = 1.0 / np.sqrt(PULSES)
    twist = np.stack([np.cos(angle) * scale, np.sin(angle) * scale]).astype(np.float32)
    phase = 2.0 * np.pi * (np.outer(q, q) % local) / local
    cosine, sine = np.cos(phase), np.sin(phase)
    both = np.concatenate(
        [np.concatenate([cosine, -sine], axis=1), np.concatenate([sine, cosine], axis=1)], axis=0
    ).astype(np.float32)
    high = both.astype(jnp.bfloat16)
    low = (both - high.astype(np.float32)).astype(jnp.bfloat16)
    return twist, high, low


def spread_kernel(x_ref, o_ref):
    parts, local, lanes = x_ref.shape
    devices = o_ref.shape[0]
    for part in range(parts):
        for start in range(0, local, LANES):
            turned = x_ref[part, start : start + LANES, :].T
            at = part * local + start
            o_ref[:, :, at : at + LANES] = turned.reshape(devices, SUBLANES, LANES)


def spread(echoes, devices, first, count):
    parts, local, _ = echoes.shape
    return pl.pallas_call(
        spread_kernel,
        grid=(count,),
        in_specs=[pl.BlockSpec((parts, local, LANES), lambda t: (0, 0, first + t))],
        out_specs=pl.BlockSpec((devices, SUBLANES, parts * local), lambda t: (0, t, 0)),
        out_shape=jax.ShapeDtypeStruct((devices, SUBLANES * count, parts * local), jnp.float32),
    )(echoes)


def rotate(real, imag, turn, count):
    if turn == 0:
        return real, imag
    if 4 * turn == count:
        return imag, -real
    cos, sin = float(np.cos(2 * np.pi * turn / count)), float(np.sin(2 * np.pi * turn / count))
    if 8 * turn == count:
        return (real + imag) * cos, (imag - real) * cos
    if 8 * turn == 3 * count:
        return (imag - real) * sin, (real + imag) * (-sin)
    return real * cos + imag * sin, imag * cos - real * sin


def radix(values):
    count = len(values)
    if count == 1:
        return values
    even, odd = radix(values[::2]), radix(values[1::2])
    top, bottom = [], []
    for i, ((er, ei), (orr, oi)) in enumerate(zip(even, odd)):
        orr, oi = rotate(orr, oi, i, count)
        top.append((er + orr, ei + oi))
        bottom.append((er - orr, ei - oi))
    return top + bottom


def exchange(values, width, lane):
    values = list(values)
    step = 1
    while step < len(values):
        shift = step * width
        low_half = (lane // shift) % 2 == 0
        for i in range(len(values)):
            if not i & step:
                a, b = values[i], values[i + step]
                values[i] = jnp.where(low_half, a, pltpu.roll(b, shift, 1))
                values[i + step] = jnp.where(low_half, pltpu.roll(a, LANES - shift, 1), b)
        step *= 2
    return values


def split(value):
    high = value.astype(jnp.bfloat16)
    return high, (value - high.astype(jnp.float32)).astype(jnp.bfloat16)


def dot(left, right):
    return jnp.dot(left, right, preferred_element_type=jnp.float32)


def transform_kernel(x_ref, twist_ref, high_ref, low_ref, o_ref, z_ref, p_ref):
    devices, rows, width = x_ref.shape
    local = width // 2
    for row in range(0, rows, SUBLANES):
        for start in range(0, local, LANES):
            re = slice(start, start + LANES)
            im = slice(local + start, local + start + LANES)
            tile = slice(row, row + SUBLANES)
            values = radix([(x_ref[d, tile, re], x_ref[d, tile, im]) for d in range(devices)])
            for k0, (real, imag) in enumerate(values):
                cos = twist_ref[0, k0 : k0 + 1, re]
                sin = twist_ref[1, k0 : k0 + 1, re]
                to = slice(k0 * rows + row, k0 * rows + row + SUBLANES)
                z_ref[to, re] = real * cos + imag * sin
                z_ref[to, im] = imag * cos - real * sin
    block = devices * rows // 2
    for start in range(0, devices * rows, block):
        high, low = split(z_ref[start : start + block, :])
        spectrum = dot(high, high_ref[...]) + dot(high, low_ref[...]) + dot(low, high_ref[...])
        real, imag = spectrum[:, :local], spectrum[:, local:]
        p_ref[start : start + block, :] = real * real + imag * imag
    group = local // devices
    inside = LANES // group
    halves = local // LANES
    lane = lax.broadcasted_iota(jnp.int32, (rows, LANES), 1)
    for upper in range(halves):
        for half in range(halves):
            mine = [
                p_ref[
                    (upper * inside + i) * rows : (upper * inside + i + 1) * rows,
                    half * LANES : (half + 1) * LANES,
                ]
                for i in range(inside)
            ]
            for i, value in enumerate(exchange(mine, group, lane)):
                o_ref[half * inside + i, upper * rows : (upper + 1) * rows, :] = value
    wide = lax.broadcasted_iota(jnp.int32, (rows, local), 1) % group
    edges = jnp.zeros((rows, local), jnp.float32)
    reach = GUARD_BINS + TRAIN_BINS
    for j in range(EDGE - reach, EDGE + reach):
        k0 = devices - EDGE + j if j < EDGE else j - EDGE
        shift = j + 1 if j < EDGE else local - group + j
        moved = pltpu.roll(p_ref[k0 * rows : (k0 + 1) * rows, :], shift, 1)
        edges = jnp.where(wide == j, moved, edges)
    small = lane[:SUBLANES]
    for half in range(halves):
        mine = [edges[row : row + SUBLANES, half * LANES : (half + 1) * LANES] for row in range(0, rows, SUBLANES)]
        mine += [jnp.zeros((SUBLANES, LANES), jnp.float32)] * (inside - len(mine))
        for i, value in enumerate(exchange(mine, group, small)):
            o_ref[half * inside + i, halves * rows : halves * rows + SUBLANES, :] = value


def transform(columns, tables):
    devices, rows, width = columns.shape
    local = width // 2
    out_rows = rows * (local // LANES) + SUBLANES
    return pl.pallas_call(
        transform_kernel,
        out_shape=jax.ShapeDtypeStruct((devices, out_rows, LANES), jnp.float32),
        scratch_shapes=[
            pltpu.VMEM((devices * rows, width), jnp.float32),
            pltpu.VMEM((devices * rows, local), jnp.float32),
        ],
    )(columns, *tables)


def finish_kernel(guard_ref, train_ref, *refs, counts, local, devices):
    blocks, (powers_ref, statistic_ref, turn_ref, pad_ref) = refs[: len(counts)], refs[len(counts) :]
    gates = powers_ref.shape[1]
    group = local // devices
    halves = local // LANES
    inside = LANES // group
    t = 0
    for count, block in zip(counts, blocks):
        rows = count * SUBLANES
        edge = block[:, halves * rows : halves * rows + SUBLANES, :].reshape(LANES, LANES).T
        for own in range(count):
            cols = slice(t * LANES, (t + 1) * LANES)
            for half in range(halves):
                at = half * rows + own * SUBLANES
                turn_ref[half, :, :] = block[:, at : at + SUBLANES, :].reshape(LANES, LANES).T
            for f1 in range(group):
                for half in range(halves):
                    tile = turn_ref[half, pl.ds(f1, inside, stride=group), :]
                    at = f1 * devices + half * inside
                    powers_ref[at : at + inside, cols] = tile
                    pad_ref[EDGE + at : EDGE + at + inside, cols] = tile
            pad_ref[0:EDGE, cols] = edge[own * group : own * group + EDGE, :]
            pad_ref[EDGE + local : 2 * EDGE + local, cols] = edge[own * group + EDGE : (own + 1) * group, :]
            t += 1
    guard, train = guard_ref[0], train_ref[0]
    source = lax.broadcasted_iota(jnp.int32, (3 * LANES, LANES), 0)
    target = lax.broadcasted_iota(jnp.int32, (3 * LANES, LANES), 1) + LANES
    offset = jnp.abs(source - target)
    band = ((offset > guard) & (offset <= guard + train)).astype(jnp.float32).astype(jnp.bfloat16)
    total = gates // LANES
    for t in range(total):
        cols = slice(t * LANES, (t + 1) * LANES)
        first, last = max(t - 1, 0), min(t + 2, total)
        near = powers_ref[:, first * LANES : last * LANES]
        part = band[(first - t + 1) * LANES : (last - t + 1) * LANES, :]
        high, low = split(near)
        sums = dot(high, part) + dot(low, part)
        pairs = pad_ref[0 : local + 2 * EDGE - 1, cols] + pad_ref[1 : local + 2 * EDGE, cols]
        fours = pairs[: local + 2 * EDGE - 3] + pairs[2:]
        near_side = EDGE + GUARD_BINS + 1
        far_side = EDGE - GUARD_BINS - TRAIN_BINS
        sums = sums + fours[near_side : near_side + local] + fours[far_side : far_side + local]
        gate = lax.broadcasted_iota(jnp.int32, (1, LANES), 1) + t * LANES
        cells = jnp.clip(gate - guard, 0, train) + jnp.clip(gates - 1 - gate - guard, 0, train)
        noise = sums / (cells.astype(jnp.float32) + 2.0 * TRAIN_BINS)
        statistic_ref[:, cols] = powers_ref[:, cols] / (noise + 1.0)


def finish(blocks, guard_gates, train_gates, counts, local, gates):
    devices = blocks[0].shape[0]
    out = jax.ShapeDtypeStruct((local, gates), jnp.float32)
    vmem = pl.BlockSpec(memory_space=pltpu.VMEM)
    smem = pl.BlockSpec(memory_space=pltpu.SMEM)

    def body(*refs):
        finish_kernel(*refs, counts=counts, local=local, devices=devices)

    return pl.pallas_call(
        body,
        in_specs=[smem, smem] + [vmem] * len(blocks),
        out_specs=[vmem, vmem],
        out_shape=[out, out],
        scratch_shapes=[
            pltpu.VMEM((local // LANES, LANES, LANES), jnp.float32),
            pltpu.VMEM((local + 2 * EDGE, gates), jnp.float32),
        ],
    )(guard_gates, train_gates, *blocks)


def shards(echoes, guard_gates, train_gates):
    devices = lax.axis_size("pulse")
    local, gates = echoes.shape[1:]
    fits = devices * SUBLANES == LANES and local == devices * 2 * EDGE
    fits = fits and gates == sum(CHUNKS) * LANES
    if not fits:
        return plain_shards(echoes, guard_gates, train_gates)
    tables = host_tables(devices, local)
    starts = [sum(CHUNKS[:i]) for i in range(len(CHUNKS))]
    columns = [
        lax.all_to_all(spread(echoes, devices, first, count), "pulse", 0, 0, tiled=True)
        for first, count in zip(starts, CHUNKS)
    ]
    blocks = [
        lax.all_to_all(transform(column, tables), "pulse", 0, 0, tiled=True) for column in columns
    ]
    return tuple(finish(blocks, guard_gates, train_gates, CHUNKS, local, gates))


def solution(mesh):
    return jax.shard_map(
        shards,
        mesh=mesh,
        in_specs=(P(None, "pulse", "beam"), P(), P()),
        out_specs=(P("pulse", "beam"), P("pulse", "beam")),
        check_vma=False,
    )
```

```python
import jax
import jax.numpy as jnp
import numpy as np
from jax import lax
from jax.experimental import pallas as pl
from jax.experimental.pallas import tpu as pltpu
from jax.sharding import PartitionSpec as P

PULSES = 4096
GUARD_BINS = 2
TRAIN_BINS = 4
LANES = 128
SUBLANES = 8
EDGE = 8
CHUNKS = (6,)


TWO_PI = 6.283185307179586


def padded_2(cells, sides, width):
    for axis, dim in sides:
        count = lax.axis_size(axis)
        head = lax.slice_in_dim(cells, 0, width, axis=dim)
        tail = lax.slice_in_dim(cells, cells.shape[dim] - width, cells.shape[dim], axis=dim)
        cells = jnp.concatenate(
            [
                lax.ppermute(tail, axis, [(i, (i + 1) % count) for i in range(count)]),
                cells,
                lax.ppermute(head, axis, [((i + 1) % count, i) for i in range(count)]),
            ],
            axis=dim,
        )
    return cells


def small_tables(count):
    index_row = jnp.arange(count, dtype=jnp.int32)
    phases = (index_row[:, None] * index_row[None, :] % count).astype(jnp.float32) * (
        TWO_PI / count
    )
    return (jnp.cos(phases), jnp.sin(phases))


def product(left, right):
    return jnp.dot(left, right, precision=lax.Precision.HIGHEST, preferred_element_type=jnp.float32)


def factored_powers(samples):
    width = samples.shape[2]
    bit_count = PULSES.bit_length() - 1
    first_radix = 2 ** (bit_count // 2)
    second_radix = PULSES // first_radix
    cos_first, sin_first = small_tables(first_radix)
    real_in = samples[0].reshape(first_radix, second_radix * width)
    imag_in = samples[1].reshape(first_radix, second_radix * width)
    real_one = (product(cos_first, real_in) + product(sin_first, imag_in)).reshape(
        first_radix, second_radix, width
    )
    imag_one = (product(cos_first, imag_in) - product(sin_first, real_in)).reshape(
        first_radix, second_radix, width
    )
    first_ids = jnp.arange(first_radix, dtype=jnp.int32)
    second_ids = jnp.arange(second_radix, dtype=jnp.int32)
    twist = (first_ids[:, None] * second_ids[None, :] % PULSES).astype(jnp.float32) * (
        TWO_PI / PULSES
    )
    twist_cos = jnp.cos(twist)[:, :, None]
    twist_sin = jnp.sin(twist)[:, :, None]
    real_two = twist_cos * real_one + twist_sin * imag_one
    imag_two = twist_cos * imag_one - twist_sin * real_one
    real_two = jnp.transpose(real_two, (1, 0, 2)).reshape(second_radix, first_radix * width)
    imag_two = jnp.transpose(imag_two, (1, 0, 2)).reshape(second_radix, first_radix * width)
    cos_second, sin_second = small_tables(second_radix)
    scale_factor = 1.0 / jnp.sqrt(jnp.float32(PULSES))
    real_out = (product(cos_second, real_two) + product(sin_second, imag_two)) * scale_factor
    imag_out = (product(cos_second, imag_two) - product(sin_second, real_two)) * scale_factor
    result = real_out * real_out + imag_out * imag_out
    return result.reshape(PULSES, width)


def plain_shards(echoes, guard_gates, train_gates):
    devices_count = lax.axis_size("pulse")
    bins_local = PULSES // devices_count
    gates_count = echoes.shape[2]
    columns = factored_powers(
        lax.all_to_all(echoes, "pulse", split_axis=2, concat_axis=1, tiled=True)
    )
    powers = lax.all_to_all(columns, "pulse", split_axis=0, concat_axis=1, tiled=True)
    reach = GUARD_BINS + TRAIN_BINS
    padded = padded_2(powers, (("pulse", 0),), reach)
    doppler_sum = jnp.zeros_like(powers)
    for shift_bins in range(GUARD_BINS + 1, reach + 1):
        above = padded[reach + shift_bins : reach + shift_bins + bins_local]
        below = padded[reach - shift_bins : reach - shift_bins + bins_local]
        doppler_sum = doppler_sum + above + below
    guard_width = guard_gates[0]
    train_width = train_gates[0]
    gate_ids = jnp.arange(gates_count, dtype=jnp.int32)
    offsets = jnp.abs(gate_ids[:, None] - gate_ids[None, :])
    band = ((offsets > guard_width) & (offsets <= guard_width + train_width)).astype(jnp.float32)
    range_sum = jnp.dot(
        powers, band, precision=lax.Precision.HIGHEST, preferred_element_type=jnp.float32
    )
    range_count = jnp.sum(band, axis=0)
    noise_level = (range_sum + doppler_sum) / (range_count[None, :] + 2.0 * TRAIN_BINS)
    statistic = powers / (noise_level + 1.0)
    return (powers, statistic)


def host_tables(devices, local):
    q = np.arange(local)
    angle = 2.0 * np.pi * np.outer(np.arange(devices), q) / PULSES
    scale = 1.0 / np.sqrt(PULSES)
    twist = np.stack([np.cos(angle) * scale, np.sin(angle) * scale]).astype(np.float32)
    phase = 2.0 * np.pi * (np.outer(q, q) % local) / local
    cosine, sine = np.cos(phase), np.sin(phase)
    both = np.concatenate(
        [np.concatenate([cosine, -sine], axis=1), np.concatenate([sine, cosine], axis=1)], axis=0
    ).astype(np.float32)
    high = both.astype(jnp.bfloat16)
    low = (both - high.astype(np.float32)).astype(jnp.bfloat16)
    return twist, high, low


def spread_kernel(x_ref, o_ref):
    parts, local, lanes = x_ref.shape
    devices = o_ref.shape[0]
    for part in range(parts):
        for start in range(0, local, LANES):
            turned = x_ref[part, start : start + LANES, :].T
            at = part * local + start
            o_ref[:, :, at : at + LANES] = turned.reshape(devices, SUBLANES, LANES)


def spread(echoes, devices, first, count):
    parts, local, _ = echoes.shape
    return pl.pallas_call(
        spread_kernel,
        grid=(count,),
        in_specs=[pl.BlockSpec((parts, local, LANES), lambda t: (0, 0, first + t))],
        out_specs=pl.BlockSpec((devices, SUBLANES, parts * local), lambda t: (0, t, 0)),
        out_shape=jax.ShapeDtypeStruct((devices, SUBLANES * count, parts * local), jnp.float32),
    )(echoes)


def rotate(real, imag, turn, count):
    if turn == 0:
        return real, imag
    if 4 * turn == count:
        return imag, -real
    cos, sin = float(np.cos(2 * np.pi * turn / count)), float(np.sin(2 * np.pi * turn / count))
    if 8 * turn == count:
        return (real + imag) * cos, (imag - real) * cos
    if 8 * turn == 3 * count:
        return (imag - real) * sin, (real + imag) * (-sin)
    return real * cos + imag * sin, imag * cos - real * sin


def radix(values):
    count = len(values)
    if count == 1:
        return values
    even, odd = radix(values[::2]), radix(values[1::2])
    top, bottom = [], []
    for i, ((er, ei), (orr, oi)) in enumerate(zip(even, odd)):
        orr, oi = rotate(orr, oi, i, count)
        top.append((er + orr, ei + oi))
        bottom.append((er - orr, ei - oi))
    return top + bottom


def exchange(values, width, lane):
    values = list(values)
    step = 1
    while step < len(values):
        shift = step * width
        low_half = (lane // shift) % 2 == 0
        for i in range(len(values)):
            if not i & step:
                a, b = values[i], values[i + step]
                values[i] = jnp.where(low_half, a, pltpu.roll(b, shift, 1))
                values[i + step] = jnp.where(low_half, pltpu.roll(a, LANES - shift, 1), b)
        step *= 2
    return values


def split(value):
    high = value.astype(jnp.bfloat16)
    return high, (value - high.astype(jnp.float32)).astype(jnp.bfloat16)


def dot(left, right):
    return jnp.dot(left, right, preferred_element_type=jnp.float32)


def transform_kernel(x_ref, twist_ref, high_ref, low_ref, o_ref, z_ref, p_ref):
    devices, rows, width = x_ref.shape
    local = width // 2
    for row in range(0, rows, SUBLANES):
        for start in range(0, local, LANES):
            re = slice(start, start + LANES)
            im = slice(local + start, local + start + LANES)
            tile = slice(row, row + SUBLANES)
            values = radix([(x_ref[d, tile, re], x_ref[d, tile, im]) for d in range(devices)])
            for k0, (real, imag) in enumerate(values):
                cos = twist_ref[0, k0 : k0 + 1, re]
                sin = twist_ref[1, k0 : k0 + 1, re]
                to = slice(k0 * rows + row, k0 * rows + row + SUBLANES)
                z_ref[to, re] = real * cos + imag * sin
                z_ref[to, im] = imag * cos - real * sin
    block = devices * rows // 2
    for start in range(0, devices * rows, block):
        high, low = split(z_ref[start : start + block, :])
        spectrum = dot(high, high_ref[...]) + dot(high, low_ref[...]) + dot(low, high_ref[...])
        real, imag = spectrum[:, :local], spectrum[:, local:]
        p_ref[start : start + block, :] = real * real + imag * imag
    group = local // devices
    inside = LANES // group
    halves = local // LANES
    lane = lax.broadcasted_iota(jnp.int32, (rows, LANES), 1)
    for upper in range(halves):
        for half in range(halves):
            mine = [
                p_ref[
                    (upper * inside + i) * rows : (upper * inside + i + 1) * rows,
                    half * LANES : (half + 1) * LANES,
                ]
                for i in range(inside)
            ]
            for i, value in enumerate(exchange(mine, group, lane)):
                o_ref[half * inside + i, upper * rows : (upper + 1) * rows, :] = value
    wide = lax.broadcasted_iota(jnp.int32, (rows, local), 1) % group
    edges = jnp.zeros((rows, local), jnp.float32)
    reach = GUARD_BINS + TRAIN_BINS
    for j in range(EDGE - reach, EDGE + reach):
        k0 = devices - EDGE + j if j < EDGE else j - EDGE
        shift = j + 1 if j < EDGE else local - group + j
        moved = pltpu.roll(p_ref[k0 * rows : (k0 + 1) * rows, :], shift, 1)
        edges = jnp.where(wide == j, moved, edges)
    small = lane[:SUBLANES]
    for half in range(halves):
        mine = [edges[row : row + SUBLANES, half * LANES : (half + 1) * LANES] for row in range(0, rows, SUBLANES)]
        mine += [jnp.zeros((SUBLANES, LANES), jnp.float32)] * (inside - len(mine))
        for i, value in enumerate(exchange(mine, group, small)):
            o_ref[half * inside + i, halves * rows : halves * rows + SUBLANES, :] = value


def transform(columns, tables):
    devices, rows, width = columns.shape
    local = width // 2
    out_rows = rows * (local // LANES) + SUBLANES
    return pl.pallas_call(
        transform_kernel,
        out_shape=jax.ShapeDtypeStruct((devices, out_rows, LANES), jnp.float32),
        scratch_shapes=[
            pltpu.VMEM((devices * rows, width), jnp.float32),
            pltpu.VMEM((devices * rows, local), jnp.float32),
        ],
    )(columns, *tables)


def finish_kernel(guard_ref, train_ref, *refs, counts, local, devices):
    blocks, (powers_ref, statistic_ref, turn_ref, pad_ref) = refs[: len(counts)], refs[len(counts) :]
    gates = powers_ref.shape[1]
    group = local // devices
    halves = local // LANES
    inside = LANES // group
    t = 0
    for count, block in zip(counts, blocks):
        rows = count * SUBLANES
        edge = block[:, halves * rows : halves * rows + SUBLANES, :].reshape(LANES, LANES).T
        for own in range(count):
            cols = slice(t * LANES, (t + 1) * LANES)
            for half in range(halves):
                at = half * rows + own * SUBLANES
                turn_ref[half, :, :] = block[:, at : at + SUBLANES, :].reshape(LANES, LANES).T
            for f1 in range(group):
                for half in range(halves):
                    tile = turn_ref[half, pl.ds(f1, inside, stride=group), :]
                    at = f1 * devices + half * inside
                    powers_ref[at : at + inside, cols] = tile
                    pad_ref[EDGE + at : EDGE + at + inside, cols] = tile
            pad_ref[0:EDGE, cols] = edge[own * group : own * group + EDGE, :]
            pad_ref[EDGE + local : 2 * EDGE + local, cols] = edge[own * group + EDGE : (own + 1) * group, :]
            t += 1
    guard, train = guard_ref[0], train_ref[0]
    source = lax.broadcasted_iota(jnp.int32, (3 * LANES, LANES), 0)
    target = lax.broadcasted_iota(jnp.int32, (3 * LANES, LANES), 1) + LANES
    offset = jnp.abs(source - target)
    band = ((offset > guard) & (offset <= guard + train)).astype(jnp.float32).astype(jnp.bfloat16)
    total = gates // LANES
    for t in range(total):
        cols = slice(t * LANES, (t + 1) * LANES)
        first, last = max(t - 1, 0), min(t + 2, total)
        near = powers_ref[:, first * LANES : last * LANES]
        part = band[(first - t + 1) * LANES : (last - t + 1) * LANES, :]
        high, low = split(near)
        sums = dot(high, part) + dot(low, part)
        pairs = pad_ref[0 : local + 2 * EDGE - 1, cols] + pad_ref[1 : local + 2 * EDGE, cols]
        fours = pairs[: local + 2 * EDGE - 3] + pairs[2:]
        near_side = EDGE + GUARD_BINS + 1
        far_side = EDGE - GUARD_BINS - TRAIN_BINS
        sums = sums + fours[near_side : near_side + local] + fours[far_side : far_side + local]
        gate = lax.broadcasted_iota(jnp.int32, (1, LANES), 1) + t * LANES
        cells = jnp.clip(gate - guard, 0, train) + jnp.clip(gates - 1 - gate - guard, 0, train)
        noise = sums / (cells.astype(jnp.float32) + 2.0 * TRAIN_BINS)
        statistic_ref[:, cols] = powers_ref[:, cols] / (noise + 1.0)


def finish(blocks, guard_gates, train_gates, counts, local, gates):
    devices = blocks[0].shape[0]
    out = jax.ShapeDtypeStruct((local, gates), jnp.float32)
    vmem = pl.BlockSpec(memory_space=pltpu.VMEM)
    smem = pl.BlockSpec(memory_space=pltpu.SMEM)

    def body(*refs):
        finish_kernel(*refs, counts=counts, local=local, devices=devices)

    return pl.pallas_call(
        body,
        in_specs=[smem, smem] + [vmem] * len(blocks),
        out_specs=[vmem, vmem],
        out_shape=[out, out],
        scratch_shapes=[
            pltpu.VMEM((local // LANES, LANES, LANES), jnp.float32),
            pltpu.VMEM((local + 2 * EDGE, gates), jnp.float32),
        ],
    )(guard_gates, train_gates, *blocks)


def shards(echoes, guard_gates, train_gates):
    devices = lax.axis_size("pulse")
    local, gates = echoes.shape[1:]
    fits = devices * SUBLANES == LANES and local == devices * 2 * EDGE
    fits = fits and gates == sum(CHUNKS) * LANES
    if not fits:
        return plain_shards(echoes, guard_gates, train_gates)
    tables = host_tables(devices, local)
    starts = [sum(CHUNKS[:i]) for i in range(len(CHUNKS))]
    columns = [
        lax.all_to_all(spread(echoes, devices, first, count), "pulse", 0, 0, tiled=True)
        for first, count in zip(starts, CHUNKS)
    ]
    blocks = [
        lax.all_to_all(transform(column, tables), "pulse", 0, 0, tiled=True) for column in columns
    ]
    return tuple(finish(blocks, guard_gates, train_gates, CHUNKS, local, gates))


def solution(mesh):
    return jax.shard_map(
        shards,
        mesh=mesh,
        in_specs=(P(None, "pulse", "beam"), P(), P()),
        out_specs=(P("pulse", "beam"), P("pulse", "beam")),
        check_vma=False,
    )
```

```python
import jax
import jax.numpy as jnp
import numpy as np
from jax import lax
from jax.experimental import pallas as pl
from jax.experimental.pallas import tpu as pltpu
from jax.sharding import PartitionSpec as P

PULSES = 4096
GUARD_BINS = 2
TRAIN_BINS = 4
LANES = 128
SUBLANES = 8
EDGE = 8


TWO_PI = 6.283185307179586


def padded_2(cells, sides, width):
    for axis, dim in sides:
        count = lax.axis_size(axis)
        head = lax.slice_in_dim(cells, 0, width, axis=dim)
        tail = lax.slice_in_dim(cells, cells.shape[dim] - width, cells.shape[dim], axis=dim)
        cells = jnp.concatenate(
            [
                lax.ppermute(tail, axis, [(i, (i + 1) % count) for i in range(count)]),
                cells,
                lax.ppermute(head, axis, [((i + 1) % count, i) for i in range(count)]),
            ],
            axis=dim,
        )
    return cells


def small_tables(count):
    index_row = jnp.arange(count, dtype=jnp.int32)
    phases = (index_row[:, None] * index_row[None, :] % count).astype(jnp.float32) * (
        TWO_PI / count
    )
    return (jnp.cos(phases), jnp.sin(phases))


def product(left, right):
    return jnp.dot(left, right, precision=lax.Precision.HIGHEST, preferred_element_type=jnp.float32)


def factored_powers(samples):
    width = samples.shape[2]
    bit_count = PULSES.bit_length() - 1
    first_radix = 2 ** (bit_count // 2)
    second_radix = PULSES // first_radix
    cos_first, sin_first = small_tables(first_radix)
    real_in = samples[0].reshape(first_radix, second_radix * width)
    imag_in = samples[1].reshape(first_radix, second_radix * width)
    real_one = (product(cos_first, real_in) + product(sin_first, imag_in)).reshape(
        first_radix, second_radix, width
    )
    imag_one = (product(cos_first, imag_in) - product(sin_first, real_in)).reshape(
        first_radix, second_radix, width
    )
    first_ids = jnp.arange(first_radix, dtype=jnp.int32)
    second_ids = jnp.arange(second_radix, dtype=jnp.int32)
    twist = (first_ids[:, None] * second_ids[None, :] % PULSES).astype(jnp.float32) * (
        TWO_PI / PULSES
    )
    twist_cos = jnp.cos(twist)[:, :, None]
    twist_sin = jnp.sin(twist)[:, :, None]
    real_two = twist_cos * real_one + twist_sin * imag_one
    imag_two = twist_cos * imag_one - twist_sin * real_one
    real_two = jnp.transpose(real_two, (1, 0, 2)).reshape(second_radix, first_radix * width)
    imag_two = jnp.transpose(imag_two, (1, 0, 2)).reshape(second_radix, first_radix * width)
    cos_second, sin_second = small_tables(second_radix)
    scale_factor = 1.0 / jnp.sqrt(jnp.float32(PULSES))
    real_out = (product(cos_second, real_two) + product(sin_second, imag_two)) * scale_factor
    imag_out = (product(cos_second, imag_two) - product(sin_second, real_two)) * scale_factor
    result = real_out * real_out + imag_out * imag_out
    return result.reshape(PULSES, width)


def plain_shards(echoes, guard_gates, train_gates):
    devices_count = lax.axis_size("pulse")
    bins_local = PULSES // devices_count
    gates_count = echoes.shape[2]
    columns = factored_powers(
        lax.all_to_all(echoes, "pulse", split_axis=2, concat_axis=1, tiled=True)
    )
    powers = lax.all_to_all(columns, "pulse", split_axis=0, concat_axis=1, tiled=True)
    reach = GUARD_BINS + TRAIN_BINS
    padded = padded_2(powers, (("pulse", 0),), reach)
    doppler_sum = jnp.zeros_like(powers)
    for shift_bins in range(GUARD_BINS + 1, reach + 1):
        above = padded[reach + shift_bins : reach + shift_bins + bins_local]
        below = padded[reach - shift_bins : reach - shift_bins + bins_local]
        doppler_sum = doppler_sum + above + below
    guard_width = guard_gates[0]
    train_width = train_gates[0]
    gate_ids = jnp.arange(gates_count, dtype=jnp.int32)
    offsets = jnp.abs(gate_ids[:, None] - gate_ids[None, :])
    band = ((offsets > guard_width) & (offsets <= guard_width + train_width)).astype(jnp.float32)
    range_sum = jnp.dot(
        powers, band, precision=lax.Precision.HIGHEST, preferred_element_type=jnp.float32
    )
    range_count = jnp.sum(band, axis=0)
    noise_level = (range_sum + doppler_sum) / (range_count[None, :] + 2.0 * TRAIN_BINS)
    statistic = powers / (noise_level + 1.0)
    return (powers, statistic)


def host_tables(devices, local):
    q = np.arange(local)
    angle = 2.0 * np.pi * np.outer(np.arange(devices), q) / PULSES
    scale = 1.0 / np.sqrt(PULSES)
    twist = np.stack([np.cos(angle) * scale, np.sin(angle) * scale]).astype(np.float32)
    phase = 2.0 * np.pi * (np.outer(q, q) % local) / local
    cosine, sine = np.cos(phase), np.sin(phase)
    both = np.concatenate(
        [np.concatenate([cosine, -sine], axis=1), np.concatenate([sine, cosine], axis=1)], axis=0
    ).astype(np.float32)
    high = both.astype(jnp.bfloat16)
    low = (both - high.astype(np.float32)).astype(jnp.bfloat16)
    return twist, high, low


def spread_kernel(me_ref, x_ref, *refs):
    outs, hold_ref = refs[:-1], refs[-1]
    parts, local, lanes = x_ref.shape
    devices = len(outs)
    for part in range(parts):
        for start in range(0, local, LANES):
            turned = x_ref[part, start : start + LANES, :].T
            at = part * local + start
            hold_ref[:, :, at : at + LANES] = turned.reshape(devices, SUBLANES, LANES)
    for shift, out in enumerate(outs):
        out[...] = hold_ref[lax.rem(me_ref[0] + shift, devices)]


def spread(echoes, devices):
    parts, local, gates = echoes.shape
    count = gates // LANES
    me = lax.axis_index("pulse").astype(jnp.int32).reshape(1)
    out = jax.ShapeDtypeStruct((SUBLANES * count, parts * local), jnp.float32)
    return pl.pallas_call(
        spread_kernel,
        grid=(count,),
        in_specs=[
            pl.BlockSpec(memory_space=pltpu.SMEM),
            pl.BlockSpec((parts, local, LANES), lambda t: (0, 0, t)),
        ],
        out_specs=[pl.BlockSpec((SUBLANES, parts * local), lambda t: (t, 0))] * devices,
        out_shape=[out] * devices,
        scratch_shapes=[pltpu.VMEM((devices, SUBLANES, parts * local), jnp.float32)],
    )(me, echoes)


def shifted(blocks):
    count = len(blocks)
    return blocks[:1] + [
        lax.ppermute(blocks[shift], "pulse", [(i, (i + shift) % count) for i in range(count)])
        for shift in range(1, count)
    ]


def rotate(real, imag, turn, count):
    if turn == 0:
        return real, imag
    if 4 * turn == count:
        return imag, -real
    cos, sin = float(np.cos(2 * np.pi * turn / count)), float(np.sin(2 * np.pi * turn / count))
    if 8 * turn == count:
        return (real + imag) * cos, (imag - real) * cos
    if 8 * turn == 3 * count:
        return (imag - real) * sin, (real + imag) * (-sin)
    return real * cos + imag * sin, imag * cos - real * sin


def radix(values):
    count = len(values)
    if count == 1:
        return values
    even, odd = radix(values[::2]), radix(values[1::2])
    top, bottom = [], []
    for i, ((er, ei), (orr, oi)) in enumerate(zip(even, odd)):
        orr, oi = rotate(orr, oi, i, count)
        top.append((er + orr, ei + oi))
        bottom.append((er - orr, ei - oi))
    return top + bottom


def exchange(values, width, lane):
    values = list(values)
    step = 1
    while step < len(values):
        shift = step * width
        low_half = (lane // shift) % 2 == 0
        for i in range(len(values)):
            if not i & step:
                a, b = values[i], values[i + step]
                values[i] = jnp.where(low_half, a, pltpu.roll(b, shift, 1))
                values[i + step] = jnp.where(low_half, pltpu.roll(a, LANES - shift, 1), b)
        step *= 2
    return values


def split(value):
    high = value.astype(jnp.bfloat16)
    return high, (value - high.astype(jnp.float32)).astype(jnp.bfloat16)


def dot(left, right):
    return jnp.dot(left, right, preferred_element_type=jnp.float32)


def transform_kernel(*refs):
    twist_ref, high_ref, low_ref, o_ref, x_ref, sems, z_ref, p_ref = refs[-8:]
    devices, rows, width = x_ref.shape
    local = width // 2
    copies = [pltpu.make_async_copy(refs[s], x_ref.at[s], sems.at[s]) for s in range(devices)]
    for copy in copies:
        copy.start()
    for copy in copies:
        copy.wait()
    for row in range(0, rows, SUBLANES):
        for start in range(0, local, LANES):
            re = slice(start, start + LANES)
            im = slice(local + start, local + start + LANES)
            tile = slice(row, row + SUBLANES)
            values = radix([(x_ref[d, tile, re], x_ref[d, tile, im]) for d in range(devices)])
            values = values[:1] + values[:0:-1]
            for k0, (real, imag) in enumerate(values):
                cos = twist_ref[0, k0 : k0 + 1, re]
                sin = twist_ref[1, k0 : k0 + 1, re]
                to = slice(k0 * rows + row, k0 * rows + row + SUBLANES)
                z_ref[to, re] = real * cos + imag * sin
                z_ref[to, im] = imag * cos - real * sin
    block = devices * rows // 2
    for start in range(0, devices * rows, block):
        high, low = split(z_ref[start : start + block, :])
        spectrum = dot(high, high_ref[...]) + dot(high, low_ref[...]) + dot(low, high_ref[...])
        real, imag = spectrum[:, :local], spectrum[:, local:]
        p_ref[start : start + block, :] = real * real + imag * imag
    group = local // devices
    inside = LANES // group
    halves = local // LANES
    lane = lax.broadcasted_iota(jnp.int32, (rows, LANES), 1)
    for upper in range(halves):
        for half in range(halves):
            mine = [
                p_ref[
                    (upper * inside + i) * rows : (upper * inside + i + 1) * rows,
                    half * LANES : (half + 1) * LANES,
                ]
                for i in range(inside)
            ]
            for i, value in enumerate(exchange(mine, group, lane)):
                o_ref[half * inside + i, upper * rows : (upper + 1) * rows, :] = value
    wide = lax.broadcasted_iota(jnp.int32, (rows, local), 1) % group
    edges = jnp.zeros((rows, local), jnp.float32)
    reach = GUARD_BINS + TRAIN_BINS
    for j in range(EDGE - reach, EDGE + reach):
        k0 = devices - EDGE + j if j < EDGE else j - EDGE
        shift = j + 1 if j < EDGE else local - group + j
        moved = pltpu.roll(p_ref[k0 * rows : (k0 + 1) * rows, :], shift, 1)
        edges = jnp.where(wide == j, moved, edges)
    small = lane[:SUBLANES]
    for half in range(halves):
        mine = [edges[row : row + SUBLANES, half * LANES : (half + 1) * LANES] for row in range(0, rows, SUBLANES)]
        mine += [jnp.zeros((SUBLANES, LANES), jnp.float32)] * (inside - len(mine))
        for i, value in enumerate(exchange(mine, group, small)):
            o_ref[half * inside + i, halves * rows : halves * rows + SUBLANES, :] = value


def transform(columns, tables):
    devices = len(columns)
    rows, width = columns[0].shape
    local = width // 2
    out_rows = rows * (local // LANES) + SUBLANES
    vmem = pl.BlockSpec(memory_space=pltpu.VMEM)
    return pl.pallas_call(
        transform_kernel,
        in_specs=[pl.BlockSpec(memory_space=pl.ANY)] * devices + [vmem] * 3,
        out_specs=vmem,
        out_shape=jax.ShapeDtypeStruct((devices, out_rows, LANES), jnp.float32),
        scratch_shapes=[
            pltpu.VMEM((devices, rows, width), jnp.float32),
            pltpu.SemaphoreType.DMA((devices,)),
            pltpu.VMEM((devices * rows, width), jnp.float32),
            pltpu.VMEM((devices * rows, local), jnp.float32),
        ],
    )(*columns, *tables)


def finish_kernel(guard_ref, train_ref, *refs, counts, local, devices):
    blocks, (powers_ref, statistic_ref, turn_ref, pad_ref) = refs[: len(counts)], refs[len(counts) :]
    gates = powers_ref.shape[1]
    group = local // devices
    halves = local // LANES
    inside = LANES // group
    t = 0
    for count, block in zip(counts, blocks):
        rows = count * SUBLANES
        edge = block[:, halves * rows : halves * rows + SUBLANES, :].reshape(LANES, LANES).T
        for own in range(count):
            cols = slice(t * LANES, (t + 1) * LANES)
            for half in range(halves):
                at = half * rows + own * SUBLANES
                turn_ref[half, :, :] = block[:, at : at + SUBLANES, :].reshape(LANES, LANES).T
            for f1 in range(group):
                for half in range(halves):
                    tile = turn_ref[half, pl.ds(f1, inside, stride=group), :]
                    at = f1 * devices + half * inside
                    powers_ref[at : at + inside, cols] = tile
                    pad_ref[EDGE + at : EDGE + at + inside, cols] = tile
            pad_ref[0:EDGE, cols] = edge[own * group : own * group + EDGE, :]
            pad_ref[EDGE + local : 2 * EDGE + local, cols] = edge[own * group + EDGE : (own + 1) * group, :]
            t += 1
    guard, train = guard_ref[0], train_ref[0]
    source = lax.broadcasted_iota(jnp.int32, (3 * LANES, LANES), 0)
    target = lax.broadcasted_iota(jnp.int32, (3 * LANES, LANES), 1) + LANES
    offset = jnp.abs(source - target)
    band = ((offset > guard) & (offset <= guard + train)).astype(jnp.float32).astype(jnp.bfloat16)
    total = gates // LANES
    for t in range(total):
        cols = slice(t * LANES, (t + 1) * LANES)
        first, last = max(t - 1, 0), min(t + 2, total)
        near = powers_ref[:, first * LANES : last * LANES]
        part = band[(first - t + 1) * LANES : (last - t + 1) * LANES, :]
        high, low = split(near)
        sums = dot(high, part) + dot(low, part)
        pairs = pad_ref[0 : local + 2 * EDGE - 1, cols] + pad_ref[1 : local + 2 * EDGE, cols]
        fours = pairs[: local + 2 * EDGE - 3] + pairs[2:]
        near_side = EDGE + GUARD_BINS + 1
        far_side = EDGE - GUARD_BINS - TRAIN_BINS
        sums = sums + fours[near_side : near_side + local] + fours[far_side : far_side + local]
        gate = lax.broadcasted_iota(jnp.int32, (1, LANES), 1) + t * LANES
        cells = jnp.clip(gate - guard, 0, train) + jnp.clip(gates - 1 - gate - guard, 0, train)
        noise = sums / (cells.astype(jnp.float32) + 2.0 * TRAIN_BINS)
        statistic_ref[:, cols] = powers_ref[:, cols] / (noise + 1.0)


def finish(blocks, guard_gates, train_gates, counts, local, gates):
    devices = blocks[0].shape[0]
    out = jax.ShapeDtypeStruct((local, gates), jnp.float32)
    vmem = pl.BlockSpec(memory_space=pltpu.VMEM)
    smem = pl.BlockSpec(memory_space=pltpu.SMEM)

    def body(*refs):
        finish_kernel(*refs, counts=counts, local=local, devices=devices)

    return pl.pallas_call(
        body,
        in_specs=[smem, smem] + [vmem] * len(blocks),
        out_specs=[vmem, vmem],
        out_shape=[out, out],
        scratch_shapes=[
            pltpu.VMEM((local // LANES, LANES, LANES), jnp.float32),
            pltpu.VMEM((local + 2 * EDGE, gates), jnp.float32),
        ],
    )(guard_gates, train_gates, *blocks)


def shards(echoes, guard_gates, train_gates):
    devices = lax.axis_size("pulse")
    local, gates = echoes.shape[1:]
    fits = devices * SUBLANES == LANES and local == devices * 2 * EDGE
    fits = fits and gates % LANES == 0 and gates // LANES <= SUBLANES
    if not fits:
        return plain_shards(echoes, guard_gates, train_gates)
    tables = host_tables(devices, local)
    block = transform(shifted(list(spread(echoes, devices))), tables)
    block = lax.all_to_all(block, "pulse", 0, 0, tiled=True)
    counts = (gates // LANES,)
    return tuple(finish([block], guard_gates, train_gates, counts, local, gates))


def solution(mesh):
    return jax.shard_map(
        shards,
        mesh=mesh,
        in_specs=(P(None, "pulse", "beam"), P(), P()),
        out_specs=(P("pulse", "beam"), P("pulse", "beam")),
        check_vma=False,
    )
```

```python
import jax
import jax.numpy as jnp
import numpy as np
from jax import lax
from jax.experimental import pallas as pl
from jax.experimental.pallas import tpu as pltpu
from jax.sharding import PartitionSpec as P

PULSES = 4096
GUARD_BINS = 2
TRAIN_BINS = 4
LANES = 128
SUBLANES = 8
EDGE = 8


TWO_PI = 6.283185307179586


def padded_2(cells, sides, width):
    for axis, dim in sides:
        count = lax.axis_size(axis)
        head = lax.slice_in_dim(cells, 0, width, axis=dim)
        tail = lax.slice_in_dim(cells, cells.shape[dim] - width, cells.shape[dim], axis=dim)
        cells = jnp.concatenate(
            [
                lax.ppermute(tail, axis, [(i, (i + 1) % count) for i in range(count)]),
                cells,
                lax.ppermute(head, axis, [((i + 1) % count, i) for i in range(count)]),
            ],
            axis=dim,
        )
    return cells


def small_tables(count):
    index_row = jnp.arange(count, dtype=jnp.int32)
    phases = (index_row[:, None] * index_row[None, :] % count).astype(jnp.float32) * (
        TWO_PI / count
    )
    return (jnp.cos(phases), jnp.sin(phases))


def product(left, right):
    return jnp.dot(left, right, precision=lax.Precision.HIGHEST, preferred_element_type=jnp.float32)


def factored_powers(samples):
    width = samples.shape[2]
    bit_count = PULSES.bit_length() - 1
    first_radix = 2 ** (bit_count // 2)
    second_radix = PULSES // first_radix
    cos_first, sin_first = small_tables(first_radix)
    real_in = samples[0].reshape(first_radix, second_radix * width)
    imag_in = samples[1].reshape(first_radix, second_radix * width)
    real_one = (product(cos_first, real_in) + product(sin_first, imag_in)).reshape(
        first_radix, second_radix, width
    )
    imag_one = (product(cos_first, imag_in) - product(sin_first, real_in)).reshape(
        first_radix, second_radix, width
    )
    first_ids = jnp.arange(first_radix, dtype=jnp.int32)
    second_ids = jnp.arange(second_radix, dtype=jnp.int32)
    twist = (first_ids[:, None] * second_ids[None, :] % PULSES).astype(jnp.float32) * (
        TWO_PI / PULSES
    )
    twist_cos = jnp.cos(twist)[:, :, None]
    twist_sin = jnp.sin(twist)[:, :, None]
    real_two = twist_cos * real_one + twist_sin * imag_one
    imag_two = twist_cos * imag_one - twist_sin * real_one
    real_two = jnp.transpose(real_two, (1, 0, 2)).reshape(second_radix, first_radix * width)
    imag_two = jnp.transpose(imag_two, (1, 0, 2)).reshape(second_radix, first_radix * width)
    cos_second, sin_second = small_tables(second_radix)
    scale_factor = 1.0 / jnp.sqrt(jnp.float32(PULSES))
    real_out = (product(cos_second, real_two) + product(sin_second, imag_two)) * scale_factor
    imag_out = (product(cos_second, imag_two) - product(sin_second, real_two)) * scale_factor
    result = real_out * real_out + imag_out * imag_out
    return result.reshape(PULSES, width)


def plain_shards(echoes, guard_gates, train_gates):
    devices_count = lax.axis_size("pulse")
    bins_local = PULSES // devices_count
    gates_count = echoes.shape[2]
    columns = factored_powers(
        lax.all_to_all(echoes, "pulse", split_axis=2, concat_axis=1, tiled=True)
    )
    powers = lax.all_to_all(columns, "pulse", split_axis=0, concat_axis=1, tiled=True)
    reach = GUARD_BINS + TRAIN_BINS
    padded = padded_2(powers, (("pulse", 0),), reach)
    doppler_sum = jnp.zeros_like(powers)
    for shift_bins in range(GUARD_BINS + 1, reach + 1):
        above = padded[reach + shift_bins : reach + shift_bins + bins_local]
        below = padded[reach - shift_bins : reach - shift_bins + bins_local]
        doppler_sum = doppler_sum + above + below
    guard_width = guard_gates[0]
    train_width = train_gates[0]
    gate_ids = jnp.arange(gates_count, dtype=jnp.int32)
    offsets = jnp.abs(gate_ids[:, None] - gate_ids[None, :])
    band = ((offsets > guard_width) & (offsets <= guard_width + train_width)).astype(jnp.float32)
    range_sum = jnp.dot(
        powers, band, precision=lax.Precision.HIGHEST, preferred_element_type=jnp.float32
    )
    range_count = jnp.sum(band, axis=0)
    noise_level = (range_sum + doppler_sum) / (range_count[None, :] + 2.0 * TRAIN_BINS)
    statistic = powers / (noise_level + 1.0)
    return (powers, statistic)


def host_tables(devices, local):
    q = np.arange(local)
    angle = 2.0 * np.pi * np.outer(np.arange(devices), q) / PULSES
    scale = 1.0 / np.sqrt(PULSES)
    twist = np.stack([np.cos(angle) * scale, np.sin(angle) * scale]).astype(np.float32)
    phase = 2.0 * np.pi * (np.outer(q, q) % local) / local
    cosine, sine = np.cos(phase), np.sin(phase)
    both = np.concatenate(
        [np.concatenate([cosine, -sine], axis=1), np.concatenate([sine, cosine], axis=1)], axis=0
    ).astype(np.float32)
    high = both.astype(jnp.bfloat16)
    low = (both - high.astype(np.float32)).astype(jnp.bfloat16)
    return twist, high, low


def spread_kernel(me_ref, x_ref, *refs):
    outs, hold_ref = refs[:-1], refs[-1]
    parts, local, lanes = x_ref.shape
    devices = len(outs)
    for part in range(parts):
        for start in range(0, local, LANES):
            turned = x_ref[part, start : start + LANES, :].T
            at = part * local + start
            hold_ref[:, :, at : at + LANES] = turned.reshape(devices, SUBLANES, LANES)
    for shift, out in enumerate(outs):
        out[...] = hold_ref[lax.rem(me_ref[0] + shift, devices)]


def spread(echoes, devices):
    parts, local, gates = echoes.shape
    count = gates // LANES
    me = lax.axis_index("pulse").astype(jnp.int32).reshape(1)
    out = jax.ShapeDtypeStruct((SUBLANES * count, parts * local), jnp.float32)
    return pl.pallas_call(
        spread_kernel,
        grid=(count,),
        in_specs=[
            pl.BlockSpec(memory_space=pltpu.SMEM),
            pl.BlockSpec((parts, local, LANES), lambda t: (0, 0, t)),
        ],
        out_specs=[pl.BlockSpec((SUBLANES, parts * local), lambda t: (t, 0))] * devices,
        out_shape=[out] * devices,
        scratch_shapes=[pltpu.VMEM((devices, SUBLANES, parts * local), jnp.float32)],
    )(me, echoes)


def shifted(blocks):
    count = len(blocks)
    moved = list(blocks)
    for shift in sorted(range(1, count), key=lambda s: abs(2 * s - count)):
        pairs = [(i, (i + shift) % count) for i in range(count)]
        moved[shift] = lax.ppermute(blocks[shift], "pulse", pairs)
    return moved


def rotate(real, imag, turn, count):
    if turn == 0:
        return real, imag
    if 4 * turn == count:
        return imag, -real
    cos, sin = float(np.cos(2 * np.pi * turn / count)), float(np.sin(2 * np.pi * turn / count))
    if 8 * turn == count:
        return (real + imag) * cos, (imag - real) * cos
    if 8 * turn == 3 * count:
        return (imag - real) * sin, (real + imag) * (-sin)
    return real * cos + imag * sin, imag * cos - real * sin


def radix(values):
    count = len(values)
    if count == 1:
        return values
    even, odd = radix(values[::2]), radix(values[1::2])
    top, bottom = [], []
    for i, ((er, ei), (orr, oi)) in enumerate(zip(even, odd)):
        orr, oi = rotate(orr, oi, i, count)
        top.append((er + orr, ei + oi))
        bottom.append((er - orr, ei - oi))
    return top + bottom


def exchange(values, width, lane):
    values = list(values)
    step = 1
    while step < len(values):
        shift = step * width
        low_half = (lane // shift) % 2 == 0
        for i in range(len(values)):
            if not i & step:
                a, b = values[i], values[i + step]
                values[i] = jnp.where(low_half, a, pltpu.roll(b, shift, 1))
                values[i + step] = jnp.where(low_half, pltpu.roll(a, LANES - shift, 1), b)
        step *= 2
    return values


def split(value):
    high = value.astype(jnp.bfloat16)
    return high, (value - high.astype(jnp.float32)).astype(jnp.bfloat16)


def dot(left, right):
    return jnp.dot(left, right, preferred_element_type=jnp.float32)


def transform_kernel(*refs):
    twist_ref, high_ref, low_ref, o_ref, x_ref, sems, z_ref, p_ref = refs[-8:]
    devices, rows, width = x_ref.shape
    local = width // 2
    copies = [pltpu.make_async_copy(refs[s], x_ref.at[s], sems.at[s]) for s in range(devices)]
    for copy in copies:
        copy.start()
    for copy in copies:
        copy.wait()
    for row in range(0, rows, SUBLANES):
        for start in range(0, local, LANES):
            re = slice(start, start + LANES)
            im = slice(local + start, local + start + LANES)
            tile = slice(row, row + SUBLANES)
            values = radix([(x_ref[d, tile, re], x_ref[d, tile, im]) for d in range(devices)])
            values = values[:1] + values[:0:-1]
            for k0, (real, imag) in enumerate(values):
                cos = twist_ref[0, k0 : k0 + 1, re]
                sin = twist_ref[1, k0 : k0 + 1, re]
                to = slice(k0 * rows + row, k0 * rows + row + SUBLANES)
                z_ref[to, re] = real * cos + imag * sin
                z_ref[to, im] = imag * cos - real * sin
    block = devices * rows // 2
    for start in range(0, devices * rows, block):
        high, low = split(z_ref[start : start + block, :])
        spectrum = dot(high, high_ref[...]) + dot(high, low_ref[...]) + dot(low, high_ref[...])
        real, imag = spectrum[:, :local], spectrum[:, local:]
        p_ref[start : start + block, :] = real * real + imag * imag
    group = local // devices
    inside = LANES // group
    halves = local // LANES
    lane = lax.broadcasted_iota(jnp.int32, (rows, LANES), 1)
    for upper in range(halves):
        for half in range(halves):
            mine = [
                p_ref[
                    (upper * inside + i) * rows : (upper * inside + i + 1) * rows,
                    half * LANES : (half + 1) * LANES,
                ]
                for i in range(inside)
            ]
            for i, value in enumerate(exchange(mine, group, lane)):
                o_ref[half * inside + i, upper * rows : (upper + 1) * rows, :] = value
    wide = lax.broadcasted_iota(jnp.int32, (rows, local), 1) % group
    edges = jnp.zeros((rows, local), jnp.float32)
    reach = GUARD_BINS + TRAIN_BINS
    for j in range(EDGE - reach, EDGE + reach):
        k0 = devices - EDGE + j if j < EDGE else j - EDGE
        shift = j + 1 if j < EDGE else local - group + j
        moved = pltpu.roll(p_ref[k0 * rows : (k0 + 1) * rows, :], shift, 1)
        edges = jnp.where(wide == j, moved, edges)
    small = lane[:SUBLANES]
    for half in range(halves):
        mine = [edges[row : row + SUBLANES, half * LANES : (half + 1) * LANES] for row in range(0, rows, SUBLANES)]
        mine += [jnp.zeros((SUBLANES, LANES), jnp.float32)] * (inside - len(mine))
        for i, value in enumerate(exchange(mine, group, small)):
            o_ref[half * inside + i, halves * rows : halves * rows + SUBLANES, :] = value


def transform(columns, tables):
    devices = len(columns)
    rows, width = columns[0].shape
    local = width // 2
    out_rows = rows * (local // LANES) + SUBLANES
    vmem = pl.BlockSpec(memory_space=pltpu.VMEM)
    return pl.pallas_call(
        transform_kernel,
        in_specs=[pl.BlockSpec(memory_space=pl.ANY)] * devices + [vmem] * 3,
        out_specs=vmem,
        out_shape=jax.ShapeDtypeStruct((devices, out_rows, LANES), jnp.float32),
        scratch_shapes=[
            pltpu.VMEM((devices, rows, width), jnp.float32),
            pltpu.SemaphoreType.DMA((devices,)),
            pltpu.VMEM((devices * rows, width), jnp.float32),
            pltpu.VMEM((devices * rows, local), jnp.float32),
        ],
    )(*columns, *tables)


def finish_kernel(guard_ref, train_ref, *refs, counts, local, devices):
    blocks, (powers_ref, statistic_ref, turn_ref, pad_ref) = refs[: len(counts)], refs[len(counts) :]
    gates = powers_ref.shape[1]
    group = local // devices
    halves = local // LANES
    inside = LANES // group
    t = 0
    for count, block in zip(counts, blocks):
        rows = count * SUBLANES
        edge = block[:, halves * rows : halves * rows + SUBLANES, :].reshape(LANES, LANES).T
        for own in range(count):
            cols = slice(t * LANES, (t + 1) * LANES)
            for half in range(halves):
                at = half * rows + own * SUBLANES
                turn_ref[half, :, :] = block[:, at : at + SUBLANES, :].reshape(LANES, LANES).T
            for f1 in range(group):
                for half in range(halves):
                    tile = turn_ref[half, pl.ds(f1, inside, stride=group), :]
                    at = f1 * devices + half * inside
                    powers_ref[at : at + inside, cols] = tile
                    pad_ref[EDGE + at : EDGE + at + inside, cols] = tile
            pad_ref[0:EDGE, cols] = edge[own * group : own * group + EDGE, :]
            pad_ref[EDGE + local : 2 * EDGE + local, cols] = edge[own * group + EDGE : (own + 1) * group, :]
            t += 1
    guard, train = guard_ref[0], train_ref[0]
    source = lax.broadcasted_iota(jnp.int32, (3 * LANES, LANES), 0)
    target = lax.broadcasted_iota(jnp.int32, (3 * LANES, LANES), 1) + LANES
    offset = jnp.abs(source - target)
    band = ((offset > guard) & (offset <= guard + train)).astype(jnp.float32).astype(jnp.bfloat16)
    total = gates // LANES
    for t in range(total):
        cols = slice(t * LANES, (t + 1) * LANES)
        first, last = max(t - 1, 0), min(t + 2, total)
        near = powers_ref[:, first * LANES : last * LANES]
        part = band[(first - t + 1) * LANES : (last - t + 1) * LANES, :]
        high, low = split(near)
        sums = dot(high, part) + dot(low, part)
        pairs = pad_ref[0 : local + 2 * EDGE - 1, cols] + pad_ref[1 : local + 2 * EDGE, cols]
        fours = pairs[: local + 2 * EDGE - 3] + pairs[2:]
        near_side = EDGE + GUARD_BINS + 1
        far_side = EDGE - GUARD_BINS - TRAIN_BINS
        sums = sums + fours[near_side : near_side + local] + fours[far_side : far_side + local]
        gate = lax.broadcasted_iota(jnp.int32, (1, LANES), 1) + t * LANES
        cells = jnp.clip(gate - guard, 0, train) + jnp.clip(gates - 1 - gate - guard, 0, train)
        noise = sums / (cells.astype(jnp.float32) + 2.0 * TRAIN_BINS)
        statistic_ref[:, cols] = powers_ref[:, cols] / (noise + 1.0)


def finish(blocks, guard_gates, train_gates, counts, local, gates):
    devices = blocks[0].shape[0]
    out = jax.ShapeDtypeStruct((local, gates), jnp.float32)
    vmem = pl.BlockSpec(memory_space=pltpu.VMEM)
    smem = pl.BlockSpec(memory_space=pltpu.SMEM)

    def body(*refs):
        finish_kernel(*refs, counts=counts, local=local, devices=devices)

    return pl.pallas_call(
        body,
        in_specs=[smem, smem] + [vmem] * len(blocks),
        out_specs=[vmem, vmem],
        out_shape=[out, out],
        scratch_shapes=[
            pltpu.VMEM((local // LANES, LANES, LANES), jnp.float32),
            pltpu.VMEM((local + 2 * EDGE, gates), jnp.float32),
        ],
    )(guard_gates, train_gates, *blocks)


def shards(echoes, guard_gates, train_gates):
    devices = lax.axis_size("pulse")
    local, gates = echoes.shape[1:]
    fits = devices * SUBLANES == LANES and local == devices * 2 * EDGE
    fits = fits and gates % LANES == 0 and gates // LANES <= SUBLANES
    if not fits:
        return plain_shards(echoes, guard_gates, train_gates)
    tables = host_tables(devices, local)
    block = transform(shifted(list(spread(echoes, devices))), tables)
    block = lax.all_to_all(block, "pulse", 0, 0, tiled=True)
    counts = (gates // LANES,)
    return tuple(finish([block], guard_gates, train_gates, counts, local, gates))


def solution(mesh):
    return jax.shard_map(
        shards,
        mesh=mesh,
        in_specs=(P(None, "pulse", "beam"), P(), P()),
        out_specs=(P("pulse", "beam"), P("pulse", "beam")),
        check_vma=False,
    )
```
